16 devices in a mesh: dp: 4 (over y, z, core), tp: 4 (over x).
Axes of the slice: x: 4, y: 2, z: 1, core: 2. Of those that a mesh axis runs over, the one named last changes fastest.
The devices are a block of a 4x4x8 slice.
Arguments:
- x: bfloat16 [8192, 8192], P('dp'), parts along dimension 0
- gain: bfloat16 [8192], replicated
- wq: bfloat16 [8192, 8192], P(None, 'tp')
- wk: bfloat16 [8192, 1024], P(None, 'tp')
- wv: bfloat16 [8192, 1024], P(None, 'tp')
- wo: bfloat16 [8192, 8192], P('tp')
Outputs:
- output: bfloat16 [8192, 8192], P('dp'), parts along dimension 0
There are 4 independent parts. The reference program is written for one: setup_inputs(seed, part) draws one part's arguments, and reference() takes and returns one part's arrays. A program takes and returns all parts, laid end to end along the dimension named above; an argument that names none is the same for every part.
All inputs are finite; a program needn't handle non-finite values.
Results may differ from the reference program's by a relative error of at most 0.012.
Values are sent between devices in bfloat16 or wider.
A program may use at most 768 MiB of HBM per device.

```python
import jax
import jax.numpy as jnp
from jax import lax

ROWS = 2048
D = 8192
HEADS = 64
KV_HEADS = 8
HEAD = 128
THETA = 10000


def setup_inputs(seed: int = 0, part: int = 0) -> dict:
    kx, kn, kq, kk, kv, ko = jax.random.split(jax.random.key(seed), 6)

    def weights(key, rows, columns):
        return jax.random.normal(key, (rows, columns), jnp.float32) * rows**-0.5

    drawn = {
        "x": jax.random.normal(jax.random.fold_in(kx, part), (ROWS, D), jnp.float32),
        "gain": 1 + 0.1 * jax.random.normal(kn, (D,), jnp.float32),
        "wq": 2 * weights(kq, D, HEADS * HEAD),
        "wk": 2 * weights(kk, D, KV_HEADS * HEAD),
        "wv": 4 * weights(kv, D, KV_HEADS * HEAD),
        "wo": weights(ko, HEADS * HEAD, D),
    }
    return {k: v.astype(jnp.bfloat16) for k, v in drawn.items()}


def normed(x, gain):
    wide = x.astype(jnp.float32)
    scale = lax.rsqrt(jnp.mean(wide * wide, -1, keepdims=True) + 1e-6)
    return (wide * scale * gain.astype(jnp.float32)).astype(jnp.bfloat16)


def turned(t, place, theta):
    half = t.shape[-1] // 2
    angle = place.astype(jnp.float32)[:, None] * theta ** (-jnp.arange(half, dtype=jnp.float32) / half)
    cos, sin = jnp.cos(angle)[:, None], jnp.sin(angle)[:, None]
    a, b = t[..., :half].astype(jnp.float32), t[..., half:].astype(jnp.float32)
    return jnp.concatenate([a * cos - b * sin, b * cos + a * sin], -1).astype(jnp.bfloat16)


def matmul(a, w):
    return jnp.dot(a, w, preferred_element_type=jnp.float32).astype(jnp.bfloat16)


def einsum(form, a, b):
    return jnp.einsum(form, a.astype(jnp.float32), b.astype(jnp.float32))


def attention(q, k, v):
    scores = einsum("tgsd,ugd->gstu", q, k) * q.shape[-1] ** -0.5
    token = jnp.arange(q.shape[0])
    scores = jnp.where(token[:, None] >= token, scores, -jnp.inf)
    weights = jax.nn.softmax(scores, -1).astype(jnp.bfloat16)
    return einsum("gstu,ugd->tgsd", weights, v).astype(jnp.bfloat16)


def reference(x, gain, wq, wk, wv, wo):
    a, place = normed(x, gain), jnp.arange(ROWS)
    q = turned(matmul(a, wq).reshape(ROWS, HEADS, HEAD), place, THETA).reshape(ROWS, KV_HEADS, -1, HEAD)
    k = turned(matmul(a, wk).reshape(ROWS, KV_HEADS, HEAD), place, THETA)
    v = matmul(a, wv).reshape(ROWS, KV_HEADS, HEAD)
    seen = attention(q, k, v).reshape(ROWS, HEADS * HEAD)
    return (x.astype(jnp.float32) + jnp.dot(seen, wo, preferred_element_type=jnp.float32)).astype(jnp.bfloat16)
```

```python
import functools

import jax
import jax.numpy as jnp
from jax import lax
from jax.experimental import pallas as pl
from jax.experimental.pallas import tpu as pltpu
from jax.sharding import PartitionSpec as P

HEAD = 128
THETA = 10000
NEG = -1e30
HIDDEN = 2 * NEG
LOG2E = 1.4426950408889634
VMEM = 67043328
R = 256
TQ = 256
TO = 512
STRIP = 512
ONES = 16
F32, BF16 = jnp.float32, jnp.bfloat16


def _dot(a, b, ca=1, cb=0):
    return lax.dot_general(a, b, (((ca,), (cb,)), ((), ())), preferred_element_type=F32)


def _kernel(n, x, gain, wq, wk, wv, wo, cos, sin, y,
            wbuf, obuf, xin, xres, a_s, q_s, k_s, v_s, top_s, mix_s, seen_s, rs1s, rs1r, rs2s, rs2r, yq,
            w_sem, o_sem, x_sem, xres_sem, own_sem, rs1_ss, rs1_rs, rs2_ss, rs2_rs, ag1_ss, ag1_rs, ag2_ss, ag2_rs):
    rows, width = x.shape
    chunks = rows // R
    quarter = width // n
    half = quarter // 2
    tiles = quarter // TO
    q_tiles = wq.shape[1] // TQ
    kv = k_s.shape[0]
    group = q_s.shape[0] // (kv * R)
    cols = group * R
    me = lax.axis_index("tp")
    right, left, far = lax.rem(me + 1, n), lax.rem(me + n - 1, n), lax.rem(me + 2, n)
    to = (right, left)

    barrier = pltpu.get_barrier_semaphore()
    for neighbour in to:
        pl.semaphore_signal(barrier, inc=1, device_id={"tp": neighbour}, device_id_type=pl.DeviceIdType.MESH)

    def remote(src, dst, send, recv, d):
        return pltpu.make_async_remote_copy(src_ref=src, dst_ref=dst, send_sem=send, recv_sem=recv, device_id={"tp": to[d]},
                                            device_id_type=pl.DeviceIdType.MESH)

    def place(j, column, size):
        return y.at[pl.ds(pl.multiple_of(j * R, R), R), pl.ds(pl.multiple_of(column, TO), size)]

    def rs1(j, d):
        s, r = lax.rem(j, 2), lax.rem(j, 4)
        return remote(rs1s.at[s, d], rs1r.at[r, d], rs1_ss.at[s, d], rs1_rs.at[r, d], d)

    def rs2(j, d):
        s, r = lax.rem(j, 2), lax.rem(j, 4)
        return remote(rs2s.at[s, d], rs2r.at[r, d], rs2_ss.at[s, d], rs2_rs.at[r, d], d)

    def ag1(j, d):
        s, r = lax.rem(j, 2), lax.rem(j, 4)
        return remote(yq.at[s], place(j, me * quarter, quarter), ag1_ss.at[s, d], ag1_rs.at[r, d], d)

    def ag2(j, d):
        s, r = lax.rem(j, 2), lax.rem(j, 4)
        here = place(j, (left, right)[d] * quarter + d * half, half)
        return remote(here, here, ag2_ss.at[s, d], ag2_rs.at[r, d], d)

    def own(j):
        s = lax.rem(j, 2)
        return pltpu.make_async_copy(yq.at[s], place(j, me * quarter, quarter), own_sem.at[s])

    def chunk_of_x(j):
        return pltpu.make_async_copy(x.at[pl.ds(pl.multiple_of(j * R, R), R), :], xin, x_sem)

    def residual(j):
        at = pl.ds(pl.multiple_of(j * R, R), R), pl.ds(pl.multiple_of(me * quarter, TO), quarter)
        return pltpu.make_async_copy(x.at[at], xres, xres_sem)

    def load(ref, column, s):
        return pltpu.make_async_copy(ref.at[:, pl.ds(pl.multiple_of(column, TQ), TQ)], wbuf.at[s], w_sem.at[s])

    def wo_load(column, s):
        return pltpu.make_async_copy(wo.at[:, pl.ds(pl.multiple_of(column, TO), TO)], obuf.at[s], o_sem.at[s])

    chunk_of_x(0).start()
    load(wk, 0, 0).start()
    load(wv, 0, 1).start()
    v_s[:, HEAD:, :] = jnp.ones((kv, ONES, rows), BF16)
    pl.semaphore_wait(barrier, 2)

    def norm(i):
        chunk_of_x(i).wait()
        part = 512

        def some(r, _):
            at = pl.ds(pl.multiple_of(r * 16, 16), 16)
            total = jnp.zeros((16, part), F32)
            for c in range(0, width, part):
                v = xin[at, c:c + part].astype(F32)
                total += v * v
            scale = lax.rsqrt(total.sum(axis=1, keepdims=True) * (1 / width) + 1e-6)
            for c in range(0, width, part):
                a_s[at, c:c + part] = (xin[at, c:c + part].astype(F32) * scale * gain[:, c:c + part]).astype(BF16)
            return None

        lax.fori_loop(0, R // 16, some, None)

        @pl.when(i + 1 < chunks)
        def _():
            chunk_of_x(i + 1).start()

    def project(s):
        return _dot(a_s[...], wbuf[s]).astype(BF16)

    def turned(t, i):
        at = pl.ds(pl.multiple_of(i * R, R), R)
        t = t.astype(F32)
        return (t * cos[at, :] + pltpu.roll(t, HEAD // 2, 1) * sin[at, :]).astype(BF16)

    def qkv(i):
        at = pl.ds(pl.multiple_of(i * R, R), R)
        load(wk, 0, 0).wait()
        t = project(0)
        load(wq, 0, 0).start()
        for j in range(kv):
            k_s[j, at, :] = turned(t[:, j * HEAD:(j + 1) * HEAD], i)
        load(wv, 0, 1).wait()
        t = project(1)
        load(wq, TQ, 1).start()
        for j in range(kv):
            v_s[j, :HEAD, at] = t[:, j * HEAD:(j + 1) * HEAD].T

        def tile(m, _):
            s = lax.rem(m, 2)
            load(wq, 0, s).wait()
            t = project(s)
            for h in range(TQ // HEAD):
                q_s[pl.ds(pl.multiple_of((m * (TQ // HEAD) + h) * R, R), R), :] = turned(t[:, h * HEAD:(h + 1) * HEAD], i)

            @pl.when(m + 2 < q_tiles)
            def _():
                load(wq, (m + 2) * TQ, s).start()

            return None

        lax.fori_loop(0, q_tiles, tile, None)

        @pl.when(i + 1 < chunks)
        def _():
            load(wk, 0, 0).start()
            load(wv, 0, 1).start()

    e = HEAD**-0.5 * LOG2E
    pieces = [(j, at) for j in range(kv) for at in range(0, cols, STRIP)]

    def attention(i):
        top_s[...] = jnp.full(top_s.shape, NEG, F32)
        mix_s[...] = jnp.zeros(mix_s.shape, F32)

        def block(b, masked):
            here = pl.ds(pl.multiple_of(b * R, R), R)
            scores = [_dot(k_s[j, here, :], q_s[j * cols + at:j * cols + at + STRIP, :], 1, 1) for j, at in pieces]
            if masked:
                query = lax.rem(lax.broadcasted_iota(jnp.int32, (R, STRIP), 1), R)
                ok = query >= lax.broadcasted_iota(jnp.int32, (R, STRIP), 0)
            weights, keeps = [], []
            for (j, at), s in zip(pieces, scores):
                if masked:
                    s = jnp.where(ok, s, HIDDEN)
                old = top_s[j:j + 1, at:at + STRIP]
                top = jnp.maximum(old, s.max(axis=0, keepdims=True))
                top_s[j:j + 1, at:at + STRIP] = top
                weights.append(jnp.exp2((s - top) * e).astype(BF16))
                keeps.append(jnp.exp2((old - top) * e))
            for (j, at), p, keep in zip(pieces, weights, keeps):
                mix_s[j, :, at:at + STRIP] = mix_s[j, :, at:at + STRIP] * keep + _dot(v_s[j, :, here], p)

        lax.fori_loop(0, i, lambda b, _: block(b, False), None)
        block(i, True)
        slot = lax.rem(i, 3)
        for j in range(kv):
            share = 1 / mix_s[j, HEAD:HEAD + 1, :]
            for g in range(group):
                seen = mix_s[j, :HEAD, g * R:(g + 1) * R] * share[:, g * R:(g + 1) * R]
                seen_s[slot, :, (j * group + g) * HEAD:(j * group + g + 1) * HEAD] = seen.T.astype(BF16)

    def prime(column):
        for t in range(2):
            wo_load(column(t), t).start()

    def over_wo(count, column, body):
        def step(t, _):
            s = lax.rem(t, 2)
            wo_load(0, s).wait()
            body(t, obuf.at[s])

            @pl.when(t + 2 < count)
            def _():
                wo_load(column(t + 2), s).start()

            return None

        lax.fori_loop(0, count, step, None)

    def column_a(t):
        return far * quarter + t * TO

    def stage_a(i):
        s = lax.rem(i, 2)
        slot = lax.rem(i, 3)
        per = tiles // 2

        def body(t, w):
            rs1s[s, t // per, lax.rem(t, per)] = _dot(seen_s[slot], w[...]).astype(BF16)
            for d in range(2):
                @pl.when(t == (d + 1) * per - 1)
                def _():
                    rs1(i, d).start()

        over_wo(tiles, column_a, body)

    def stage_b(i):
        s, r = lax.rem(i, 2), lax.rem(i, 4)
        slot = lax.rem(i, 3)
        per = tiles // 2

        def column(t):
            return jnp.where(t < tiles, right, left) * quarter + lax.rem(t, tiles) * TO

        prime(column)
        for d in range(2):
            rs1(i, d).wait_recv()

        def body(t, w):
            d, m = t // tiles, lax.rem(t, tiles)
            adds = m // per == d

            @pl.when(adds)
            def _():
                rs2s[s, d, m] = (_dot(seen_s[slot], w[...]) + rs1r[r, d, lax.rem(m, per)].astype(F32)).astype(BF16)

            @pl.when(jnp.logical_not(adds))
            def _():
                rs2s[s, d, m] = _dot(seen_s[slot], w[...]).astype(BF16)

            for d in range(2):
                @pl.when(t == (d + 1) * tiles - 1)
                def _():
                    rs2(i, d).start()

        over_wo(2 * tiles, column, body)

    def stage_c(i):
        s, r = lax.rem(i, 2), lax.rem(i, 4)
        slot = lax.rem(i, 3)

        def column(t):
            return me * quarter + t * TO

        prime(column)
        residual(i).wait()
        for d in range(2):
            rs2(i, d).wait_recv()

        def body(t, w):
            at = pl.ds(pl.multiple_of(t * TO, TO), TO)
            total = _dot(seen_s[slot], w[...]) + rs2r[r, 0, t].astype(F32) + rs2r[r, 1, t].astype(F32)
            yq[s, :, at] = (xres[:, at].astype(F32) + total).astype(BF16)

        over_wo(tiles, column, body)
        for d in range(2):
            ag1(i, d).start()
        own(i).start()

    def iteration(i, _):
        def when(first, do):
            j = i - first

            @pl.when((j >= 0) & (j < chunks))
            def _():
                do(j)

        def rs1_sent(j):
            for d in range(2):
                rs1(j, d).wait_send()

        def rs2_sent(j):
            for d in range(2):
                rs2(j, d).wait_send()

        def ag1_sent(j):
            for d in range(2):
                ag1(j, d).wait_send()
            own(j).wait()

        def forward(j):
            for d in range(2):
                ag1(j, d).wait_recv()
                ag2(j, d).start()

        def end(j):
            for d in range(2):
                ag2(j, d).wait()

        def front(j):
            norm(j)
            qkv(j)
            prime(column_a)
            attention(j)

        when(2, lambda j: residual(j).start())
        when(0, front)
        when(2, rs1_sent)
        when(0, stage_a)
        when(3, rs2_sent)
        when(1, stage_b)
        when(4, ag1_sent)
        when(2, stage_c)
        when(3, forward)
        when(4, end)
        return None

    lax.fori_loop(0, chunks + 4, iteration, None)


def solution(mesh):
    n = mesh.shape["tp"]

    def step(x, gain, wq, wk, wv, wo):
        rows, width = x.shape
        half = HEAD // 2
        kv, heads = wk.shape[1] // HEAD, wq.shape[1] // HEAD
        cols = heads // kv * R
        tiles = width // n // TO
        angle = jnp.arange(rows, dtype=F32)[:, None] * THETA ** (-jnp.arange(half, dtype=F32) / half)
        cos, sin = jnp.cos(angle), jnp.sin(angle)
        hbm, vmem = pl.BlockSpec(memory_space=pl.ANY), pl.BlockSpec(memory_space=pltpu.VMEM)
        dma = pltpu.SemaphoreType.DMA
        return pl.pallas_call(
            functools.partial(_kernel, n),
            out_shape=jax.ShapeDtypeStruct(x.shape, BF16),
            in_specs=[hbm, vmem, hbm, hbm, hbm, hbm, vmem, vmem],
            out_specs=hbm,
            scratch_shapes=[
                pltpu.VMEM((2, width, TQ), BF16),
                pltpu.VMEM((2, wo.shape[0], TO), BF16),
                pltpu.VMEM((R, width), BF16),
                pltpu.VMEM((R, width // n), BF16),
                pltpu.VMEM((R, width), BF16),
                pltpu.VMEM((heads * R, HEAD), BF16),
                pltpu.VMEM((kv, rows, HEAD), BF16),
                pltpu.VMEM((kv, HEAD + ONES, rows), BF16),
                pltpu.VMEM((kv, cols), F32),
                pltpu.VMEM((kv, HEAD + ONES, cols), F32),
                pltpu.VMEM((3, R, heads * HEAD), BF16),
                pltpu.VMEM((2, 2, tiles // 2, R, TO), BF16),
                pltpu.VMEM((4, 2, tiles // 2, R, TO), BF16),
                pltpu.VMEM((2, 2, tiles, R, TO), BF16),
                pltpu.VMEM((4, 2, tiles, R, TO), BF16),
                pltpu.VMEM((2, R, width // n), BF16),
                dma((2,)), dma((2,)), dma, dma, dma((2,)),
                dma((2, 2)), dma((4, 2)), dma((2, 2)), dma((4, 2)), dma((2, 2)), dma((4, 2)), dma((2, 2)), dma((4, 2)),
            ],
            compiler_params=pltpu.CompilerParams(collective_id=0, has_side_effects=True, vmem_limit_bytes=VMEM),
        )(x, gain.astype(F32)[None], wq, wk, wv, wo, jnp.concatenate([cos, cos], 1), jnp.concatenate([-sin, sin], 1))

    tokens, columns = P("dp", None), P(None, "tp")
    return jax.shard_map(
        step,
        mesh=mesh,
        in_specs=(tokens, P(None), columns, columns, columns, P("tp", None)),
        out_specs=tokens,
        check_vma=False,
    )
```

```python
import functools

import jax
import jax.numpy as jnp
import numpy as np
from jax import lax
from jax.experimental import pallas as pl
from jax.experimental.pallas import tpu as pltpu
from jax.sharding import PartitionSpec as P

HEAD = 128
THETA = 10000
NEG = -1e30
HIDDEN = 2 * NEG
LOG2E = 1.4426950408889634
VMEM = 67043328
R = 256
TO = 512
SLOTS = 6
STRIP = 512
ONES = 16
F32, BF16 = jnp.float32, jnp.bfloat16


def _dot(a, b, ca=1, cb=0):
    return lax.dot_general(a, b, (((ca,), (cb,)), ((), ())), preferred_element_type=F32)


def _kernel(n, x, gain, wq, wk, wv, wo, freq, y,
            cos, sin, wbuf, acc_s, xin, xres, a_s, q_s, k_s, v_s, top_s, mix_s, seen_s, rs1s, rs1r, rs2s, rs2r, yq,
            w_sem, x_sem, xres_sem, own_sem, rs1_ss, rs1_rs, rs2_ss, rs2_rs, ag1_ss, ag1_rs, ag2_ss, ag2_rs):
    rows, width = x.shape
    chunks = rows // R
    quarter = width // n
    half = quarter // 2
    tiles = quarter // TO
    deep = wo.shape[0]
    steps = width // deep
    kv = k_s.shape[0]
    group = q_s.shape[0] // (kv * R)
    cols = group * R
    me = lax.axis_index("tp")
    right, left, far = lax.rem(me + 1, n), lax.rem(me + n - 1, n), lax.rem(me + 2, n)
    to = (right, left)

    barrier = pltpu.get_barrier_semaphore()
    for neighbour in to:
        pl.semaphore_signal(barrier, inc=1, device_id={"tp": neighbour}, device_id_type=pl.DeviceIdType.MESH)

    def remote(src, dst, send, recv, d):
        return pltpu.make_async_remote_copy(src_ref=src, dst_ref=dst, send_sem=send, recv_sem=recv, device_id={"tp": to[d]},
                                            device_id_type=pl.DeviceIdType.MESH)

    def place(j, column, size):
        return y.at[pl.ds(pl.multiple_of(j * R, R), R), pl.ds(pl.multiple_of(column, TO), size)]

    def rs1(j, d):
        s, r = lax.rem(j, 2), lax.rem(j, 4)
        return remote(rs1s.at[s, d], rs1r.at[r, d], rs1_ss.at[s, d], rs1_rs.at[r, d], d)

    def rs2(j, d):
        s, r = lax.rem(j, 2), lax.rem(j, 4)
        return remote(rs2s.at[s, d], rs2r.at[r, d], rs2_ss.at[s, d], rs2_rs.at[r, d], d)

    def ag1(j, d):
        s, r = lax.rem(j, 2), lax.rem(j, 4)
        return remote(yq.at[s], place(j, me * quarter, quarter), ag1_ss.at[s, d], ag1_rs.at[r, d], d)

    def ag2(j, d):
        s, r = lax.rem(j, 2), lax.rem(j, 4)
        here = place(j, (left, right)[d] * quarter + d * half, half)
        return remote(here, here, ag2_ss.at[s, d], ag2_rs.at[r, d], d)

    def own(j):
        s = lax.rem(j, 2)
        return pltpu.make_async_copy(yq.at[s], place(j, me * quarter, quarter), own_sem.at[s])

    def chunk_of_x(j):
        return pltpu.make_async_copy(x.at[pl.ds(pl.multiple_of(j * R, R), R), :], xin, x_sem)

    def residual(j):
        at = pl.ds(pl.multiple_of(j * R, R), R), pl.ds(pl.multiple_of(me * quarter, TO), quarter)
        return pltpu.make_async_copy(x.at[at], xres, xres_sem)

    n_qkv, n_q = steps, steps * (wq.shape[1] // TO)
    at_a = n_qkv + n_q
    at_b = at_a + tiles
    at_c = at_b + 2 * tiles
    every = at_c + tiles

    def column_b(t):
        return jnp.where(t < tiles, right, left) * quarter + lax.rem(t, tiles) * TO

    def column_a(t):
        return far * quarter + t * TO

    def column_c(t):
        return me * quarter + t * TO

    def fetch(ref, row, column, dst, slot):
        pltpu.make_async_copy(ref.at[pl.ds(pl.multiple_of(row, 16), deep), pl.ds(pl.multiple_of(column, 128), dst.shape[1])], dst,
                              w_sem.at[slot]).start()

    def fetch_kv(t, slot):
        fetch(wk, t * deep, 0, wbuf.at[slot, :, :TO // 2], slot)
        fetch(wv, t * deep, 0, wbuf.at[slot, :, TO // 2:], slot)

    def fetch_q(t, slot):
        fetch(wq, lax.rem(t, steps) * deep, t // steps * TO, wbuf.at[slot], slot)

    def fetch_o(column):
        return lambda t, slot: fetch(wo, 0, column(t), wbuf.at[slot], slot)

    order = [(0, n_qkv, 0, fetch_kv), (n_qkv, at_a, 0, fetch_q), (at_a, at_b, 0, fetch_o(column_a)), (at_b, at_c, 1, fetch_o(column_b)),
             (at_c, every, 2, fetch_o(column_c))]

    def live(i, first):
        return (i >= first) & (i < chunks + first)

    def issue(i, p, low, high):
        for later in range(2):
            for start, stop, first, do in order:
                start, stop = start + later * every, stop + later * every
                if start < high and stop > low:
                    @pl.when((p >= start) & (p < stop) & live(i + later, first))
                    def _():
                        do(p - start, lax.rem(p, SLOTS))

    def arrived(p):
        slot = lax.rem(p, SLOTS)
        pltpu.make_async_copy(wo.at[:, :TO], wbuf.at[slot], w_sem.at[slot]).wait()
        return wbuf[slot]

    chunk_of_x(0).start()
    for p in range(SLOTS):
        issue(jnp.int32(0), jnp.int32(p), p, p + 1)
    v_s[:, HEAD:, :] = jnp.ones((kv, ONES, rows), BF16)
    pl.semaphore_wait(barrier, 2)

    def norm(i):
        chunk_of_x(i).wait()
        part = 512

        def some(r, _):
            at = pl.ds(pl.multiple_of(r * 16, 16), 16)
            total = jnp.zeros((16, part), F32)
            for c in range(0, width, part):
                v = xin[at, c:c + part].astype(F32)
                total += v * v
            scale = lax.rsqrt(total.sum(axis=1, keepdims=True) * (1 / width) + 1e-6)
            for c in range(0, width, part):
                a_s[at, c:c + part] = (xin[at, c:c + part].astype(F32) * scale * gain[:, c:c + part].astype(F32)).astype(BF16)
            return None

        lax.fori_loop(0, R // 16, some, None)

        @pl.when(i + 1 < chunks)
        def _():
            chunk_of_x(i + 1).start()

    def table(i):
        angle = (i * R + lax.broadcasted_iota(jnp.int32, (R, HEAD), 0)).astype(F32) * freq[...]
        low = lax.broadcasted_iota(jnp.int32, (R, HEAD), 1) < HEAD // 2
        sine = jnp.sin(angle)
        cos[...] = jnp.cos(angle)
        sin[...] = jnp.where(low, -sine, sine)

    def turned(t):
        t = t.astype(F32)
        return (t * cos[...] + pltpu.roll(t, HEAD // 2, 1) * sin[...]).astype(BF16)

    def project(i, p, low, high):
        for k in range(steps):
            part = _dot(a_s[:, k * deep:(k + 1) * deep], arrived(p + k))
            acc_s[...] = part if k == 0 else acc_s[...] + part
            issue(i, p + k + SLOTS, low + k + SLOTS, high + k + SLOTS)
        return acc_s[...].astype(BF16)

    def qkv(i):
        at = pl.ds(pl.multiple_of(i * R, R), R)
        t = project(i, jnp.int32(0), 0, 1)
        for j in range(kv):
            k_s[j, at, :] = turned(t[:, j * HEAD:(j + 1) * HEAD])
            v_s[j, :HEAD, at] = t[:, (kv + j) * HEAD:(kv + j + 1) * HEAD].T

        def tile(m, _):
            t = project(i, n_qkv + m * steps, n_qkv, at_a - steps + 1)
            for h in range(TO // HEAD):
                q_s[pl.ds(pl.multiple_of((m * (TO // HEAD) + h) * R, R), R), :] = turned(t[:, h * HEAD:(h + 1) * HEAD])
            return None

        lax.fori_loop(0, n_q // steps, tile, None)

    e = HEAD**-0.5 * LOG2E
    pieces = [(j, at) for j in range(kv) for at in range(0, cols, STRIP)]

    def attention(i):
        top_s[...] = jnp.full(top_s.shape, NEG, F32)
        mix_s[...] = jnp.zeros(mix_s.shape, F32)

        def block(b, masked):
            here = pl.ds(pl.multiple_of(b * R, R), R)
            scores = [_dot(k_s[j, here, :], q_s[j * cols + at:j * cols + at + STRIP, :], 1, 1) for j, at in pieces]
            if masked:
                query = lax.rem(lax.broadcasted_iota(jnp.int32, (R, STRIP), 1), R)
                ok = query >= lax.broadcasted_iota(jnp.int32, (R, STRIP), 0)
            weights, keeps = [], []
            for (j, at), s in zip(pieces, scores):
                if masked:
                    s = jnp.where(ok, s, HIDDEN)
                old = top_s[j:j + 1, at:at + STRIP]
                top = jnp.maximum(old, s.max(axis=0, keepdims=True))
                top_s[j:j + 1, at:at + STRIP] = top
                weights.append(jnp.exp2((s - top) * e).astype(BF16))
                keeps.append(jnp.exp2((old - top) * e))
            for (j, at), p, keep in zip(pieces, weights, keeps):
                mix_s[j, :, at:at + STRIP] = mix_s[j, :, at:at + STRIP] * keep + _dot(v_s[j, :, here], p)

        lax.fori_loop(0, i, lambda b, _: block(b, False), None)
        block(i, True)
        slot = lax.rem(i, 3)
        for j in range(kv):
            share = 1 / mix_s[j, HEAD:HEAD + 1, :]
            for g in range(group):
                seen = mix_s[j, :HEAD, g * R:(g + 1) * R] * share[:, g * R:(g + 1) * R]
                seen_s[slot, :, (j * group + g) * HEAD:(j * group + g + 1) * HEAD] = seen.T.astype(BF16)

    def over_wo(i, first, start, count, before, body, after):
        j = i - first

        @pl.when(live(i, first))
        def _():
            before(j)

        def step(t, _):
            p = start + t

            @pl.when(live(i, first))
            def _():
                body(j, t, arrived(p))

            issue(i, p + SLOTS, start + SLOTS, start + count + SLOTS)
            return None

        lax.fori_loop(0, count, step, None)

        @pl.when(live(i, first))
        def _():
            after(j)

    per = tiles // 2

    def nothing(j):
        pass

    def body_a(j, t, w):
        s = lax.rem(j, 2)
        rs1s[s, t // per, lax.rem(t, per)] = _dot(seen_s[lax.rem(j, 3)], w).astype(BF16)
        for d in range(2):
            @pl.when(t == (d + 1) * per - 1)
            def _():
                rs1(j, d).start()

    def before_b(j):
        for d in range(2):
            rs1(j, d).wait_recv()

    def body_b(j, t, w):
        s, r = lax.rem(j, 2), lax.rem(j, 4)
        d, m = t // tiles, lax.rem(t, tiles)
        adds = m // per == d

        @pl.when(adds)
        def _():
            rs2s[s, d, m] = (_dot(seen_s[lax.rem(j, 3)], w) + rs1r[r, d, lax.rem(m, per)].astype(F32)).astype(BF16)

        @pl.when(jnp.logical_not(adds))
        def _():
            rs2s[s, d, m] = _dot(seen_s[lax.rem(j, 3)], w).astype(BF16)

        for d in range(2):
            @pl.when(t == (d + 1) * tiles - 1)
            def _():
                rs2(j, d).start()

    def before_c(j):
        residual(j).wait()
        for d in range(2):
            rs2(j, d).wait_recv()

    def body_c(j, t, w):
        s, r = lax.rem(j, 2), lax.rem(j, 4)
        at = pl.ds(pl.multiple_of(t * TO, TO), TO)
        total = _dot(seen_s[lax.rem(j, 3)], w) + rs2r[r, 0, t].astype(F32) + rs2r[r, 1, t].astype(F32)
        yq[s, :, at] = (xres[:, at].astype(F32) + total).astype(BF16)

    def after_c(j):
        for d in range(2):
            ag1(j, d).start()
        own(j).start()

    def iteration(i, _):
        def when(first, do):
            @pl.when(live(i, first))
            def _():
                do(i - first)

        def rs1_sent(j):
            for d in range(2):
                rs1(j, d).wait_send()

        def rs2_sent(j):
            for d in range(2):
                rs2(j, d).wait_send()

        def ag1_sent(j):
            for d in range(2):
                ag1(j, d).wait_send()
            own(j).wait()

        def forward(j):
            for d in range(2):
                ag1(j, d).wait_recv()
                ag2(j, d).start()

        def end(j):
            for d in range(2):
                ag2(j, d).wait()

        def front(j):
            table(j)
            norm(j)
            qkv(j)

        when(2, lambda j: residual(j).start())
        when(0, front)

        @pl.when(i >= chunks)
        def _():
            for p in range(SLOTS, at_a + SLOTS):
                issue(i, jnp.int32(p), max(p, at_b), p + 1)

        when(2, rs1_sent)
        when(0, attention)
        over_wo(i, 0, at_a, tiles, nothing, body_a, nothing)
        when(3, rs2_sent)
        over_wo(i, 1, at_b, 2 * tiles, before_b, body_b, nothing)
        when(4, ag1_sent)
        over_wo(i, 2, at_c, tiles, before_c, body_c, after_c)
        when(3, forward)
        when(4, end)
        return None

    lax.fori_loop(0, chunks + 4, iteration, None)


def solution(mesh):
    n = mesh.shape["tp"]

    def step(x, gain, wq, wk, wv, wo):
        rows, width = x.shape
        half = HEAD // 2
        freq = THETA ** (-(np.arange(HEAD) % half) / half)
        kv, heads = wk.shape[1] // HEAD, wq.shape[1] // HEAD
        cols = heads // kv * R
        tiles = width // n // TO
        hbm, vmem = pl.BlockSpec(memory_space=pl.ANY), pl.BlockSpec(memory_space=pltpu.VMEM)
        dma = pltpu.SemaphoreType.DMA
        return pl.pallas_call(
            functools.partial(_kernel, n),
            out_shape=jax.ShapeDtypeStruct(x.shape, BF16),
            in_specs=[hbm, vmem, hbm, hbm, hbm, hbm, vmem],
            out_specs=hbm,
            scratch_shapes=[
                pltpu.VMEM((R, HEAD), F32),
                pltpu.VMEM((R, HEAD), F32),
                pltpu.VMEM((SLOTS, wo.shape[0], TO), BF16),
                pltpu.VMEM((R, TO), F32),
                pltpu.VMEM((R, width), BF16),
                pltpu.VMEM((R, width // n), BF16),
                pltpu.VMEM((R, width), BF16),
                pltpu.VMEM((heads * R, HEAD), BF16),
                pltpu.VMEM((kv, rows, HEAD), BF16),
                pltpu.VMEM((kv, HEAD + ONES, rows), BF16),
                pltpu.VMEM((kv, cols), F32),
                pltpu.VMEM((kv, HEAD + ONES, cols), F32),
                pltpu.VMEM((3, R, heads * HEAD), BF16),
                pltpu.VMEM((2, 2, tiles // 2, R, TO), BF16),
                pltpu.VMEM((4, 2, tiles // 2, R, TO), BF16),
                pltpu.VMEM((2, 2, tiles, R, TO), BF16),
                pltpu.VMEM((4, 2, tiles, R, TO), BF16),
                pltpu.VMEM((2, R, width // n), BF16),
                dma((SLOTS,)), dma, dma, dma((2,)),
                dma((2, 2)), dma((4, 2)), dma((2, 2)), dma((4, 2)), dma((2, 2)), dma((4, 2)), dma((2, 2)), dma((4, 2)),
            ],
            compiler_params=pltpu.CompilerParams(collective_id=0, has_side_effects=True, vmem_limit_bytes=VMEM),
        )(x, gain[None], wq, wk, wv, wo, jnp.asarray(freq, F32)[None])

    tokens, columns = P("dp", None), P(None, "tp")
    return jax.shard_map(
        step,
        mesh=mesh,
        in_specs=(tokens, P(None), columns, columns, columns, P("tp", None)),
        out_specs=tokens,
        check_vma=False,
    )
```

```python
import functools

import jax
import jax.numpy as jnp
import numpy as np
from jax import lax
from jax.experimental import pallas as pl
from jax.experimental.pallas import tpu as pltpu
from jax.sharding import PartitionSpec as P

HEAD = 128
THETA = 10000
NEG = -1e30
HIDDEN = 2 * NEG
LOG2E = 1.4426950408889634
VMEM = 67043328
R = 256
TO = 512
SLOTS = 6
STRIP = 512
ONES = 16
F32, BF16 = jnp.float32, jnp.bfloat16


def _dot(a, b, ca=1, cb=0):
    return lax.dot_general(a, b, (((ca,), (cb,)), ((), ())), preferred_element_type=F32)


def _kernel(n, x, gain, wq, wk, wv, wo, freq, y,
            cos, sin, gain_s, wbuf, acc_s, xin, xres, a_s, q_s, k_s, v_s, top_s, mix_s, seen_s, rs1s, rs1r, rs2s, rs2r, yq,
            w_sem, x_sem, xres_sem, own_sem, rs1_ss, rs1_rs, rs2_ss, rs2_rs, ag1_ss, ag1_rs, ag2_ss, ag2_rs):
    rows, width = x.shape
    chunks = rows // R
    quarter = width // n
    half = quarter // 2
    tiles = quarter // TO
    per = tiles // 2
    deep = wo.shape[0]
    steps = width // deep
    kv = k_s.shape[0]
    group = q_s.shape[0] // (kv * R)
    cols = group * R
    me = lax.axis_index("tp")
    right, left, far = lax.rem(me + 1, n), lax.rem(me + n - 1, n), lax.rem(me + 2, n)
    to = (right, left)

    barrier = pltpu.get_barrier_semaphore()
    for neighbour in to:
        pl.semaphore_signal(barrier, inc=1, device_id={"tp": neighbour}, device_id_type=pl.DeviceIdType.MESH)

    def remote(src, dst, send, recv, d):
        return pltpu.make_async_remote_copy(src_ref=src, dst_ref=dst, send_sem=send, recv_sem=recv, device_id={"tp": jnp.where(d == 0, right, left)},
                                            device_id_type=pl.DeviceIdType.MESH)

    def place(j, column, size):
        return y.at[pl.ds(pl.multiple_of(j * R, R), R), pl.ds(pl.multiple_of(column, TO), size)]

    def rs1(j, d, m):
        s, r = lax.rem(j, 2), lax.rem(j, 4)
        return remote(rs1s.at[s, d, m], rs1r.at[r, d, m], rs1_ss.at[s, d, m], rs1_rs.at[r, d, m], d)

    def rs2(j, d, adds):
        s, r = lax.rem(j, 2), lax.rem(j, 4)
        at = pl.ds((d if adds else 1 - d) * per, per)
        return remote(rs2s.at[s, d, at], rs2r.at[r, d, at], rs2_ss.at[s, d, adds], rs2_rs.at[r, d, adds], d)

    def ag1(j, d):
        s, r = lax.rem(j, 2), lax.rem(j, 4)
        return remote(yq.at[s], place(j, me * quarter, quarter), ag1_ss.at[s, d], ag1_rs.at[r, d], d)

    def ag2(j, d):
        s, r = lax.rem(j, 2), lax.rem(j, 4)
        here = place(j, (left, right)[d] * quarter + d * half, half)
        return remote(here, here, ag2_ss.at[s, d], ag2_rs.at[r, d], d)

    def own(j):
        s = lax.rem(j, 2)
        return pltpu.make_async_copy(yq.at[s], place(j, me * quarter, quarter), own_sem.at[s])

    def chunk_of_x(j):
        return pltpu.make_async_copy(x.at[pl.ds(pl.multiple_of(j * R, R), R), :], xin, x_sem)

    def residual(j):
        at = pl.ds(pl.multiple_of(j * R, R), R), pl.ds(pl.multiple_of(me * quarter, TO), quarter)
        return pltpu.make_async_copy(x.at[at], xres, xres_sem)

    columns_q = wq.shape[1] // TO
    early = columns_q // 2
    at_q = steps
    at_b = at_q + steps * early
    at_rest = at_b + tiles
    at_a = at_rest + steps * (columns_q - early)
    at_free = at_a + tiles
    at_c = at_free + tiles
    every = at_c + tiles

    def column_a(t):
        return far * quarter + (lax.rem(t, 2) * per + t // 2) * TO

    def column_free(t):
        return jnp.where(t < per, right, left) * quarter + (jnp.where(t < per, per, 0) + lax.rem(t, per)) * TO

    def column_b(t):
        return jnp.where(t < per, right, left) * quarter + t * TO

    def column_c(t):
        return me * quarter + t * TO

    def fetch(ref, row, column, dst, slot):
        pltpu.make_async_copy(ref.at[pl.ds(pl.multiple_of(row, 16), deep), pl.ds(pl.multiple_of(column, 128), dst.shape[1])], dst,
                              w_sem.at[slot]).start()

    def fetch_kv(t, slot):
        fetch(wk, t * deep, 0, wbuf.at[slot, :, :TO // 2], slot)
        fetch(wv, t * deep, 0, wbuf.at[slot, :, TO // 2:], slot)

    def fetch_q(first):
        return lambda t, slot: fetch(wq, lax.rem(t, steps) * deep, (first + t // steps) * TO, wbuf.at[slot], slot)

    def fetch_o(column):
        return lambda t, slot: fetch(wo, 0, column(t), wbuf.at[slot], slot)

    def live(i, first):
        return (i >= first) & (i < chunks + first)

    order = [(0, at_q, 0, fetch_kv), (at_q, at_b, 0, fetch_q(0)), (at_b, at_rest, 1, fetch_o(column_b)),
             (at_rest, at_a, 0, fetch_q(early)), (at_a, at_free, 0, fetch_o(column_a)), (at_free, at_c, 0, fetch_o(column_free)),
             (at_c, every, 2, fetch_o(column_c))]

    def issue(i, p, low, high):
        for later in range(2):
            for start, stop, first, do in order:
                start, stop = start + later * every, stop + later * every
                if start < high and stop > low:
                    @pl.when((p >= start) & (p < stop) & live(i + later, first))
                    def _():
                        do(p - start, lax.rem(p, SLOTS))

    def arrived(p):
        slot = lax.rem(p, SLOTS)
        pltpu.make_async_copy(wo.at[:, :TO], wbuf.at[slot], w_sem.at[slot]).wait()
        return wbuf[slot]

    chunk_of_x(0).start()
    for p in range(SLOTS):
        issue(jnp.int32(0), jnp.int32(p), p, p + 1)
    v_s[:, HEAD:, :] = jnp.ones((kv, ONES, rows), BF16)
    wide = gain[...].astype(F32)
    for c in range(width // 128):
        gain_s[:, c * 128:(c + 1) * 128] = wide[c:c + 1, :]
    pl.semaphore_wait(barrier, 2)

    def norm(i):
        chunk_of_x(i).wait()
        part = 512

        def some(r, _):
            at = pl.ds(pl.multiple_of(r * 16, 16), 16)
            total = jnp.zeros((16, part), F32)
            for c in range(0, width, part):
                v = xin[at, c:c + part].astype(F32)
                total += v * v
            scale = lax.rsqrt(total.sum(axis=1, keepdims=True) * (1 / width) + 1e-6)
            for c in range(0, width, part):
                a_s[at, c:c + part] = (xin[at, c:c + part].astype(F32) * scale * gain_s[:, c:c + part]).astype(BF16)
            return None

        lax.fori_loop(0, R // 16, some, None)

        @pl.when(i + 1 < chunks)
        def _():
            chunk_of_x(i + 1).start()

    def table(i):
        angle = (i * R + lax.broadcasted_iota(jnp.int32, (R, HEAD), 0)).astype(F32) * freq[...]
        low = lax.broadcasted_iota(jnp.int32, (R, HEAD), 1) < HEAD // 2
        sine = jnp.sin(angle)
        cos[...] = jnp.cos(angle)
        sin[...] = jnp.where(low, -sine, sine)

    def turned(t):
        t = t.astype(F32)
        return (t * cos[...] + pltpu.roll(t, HEAD // 2, 1) * sin[...]).astype(BF16)

    def project(i, p, low, high):
        for k in range(steps):
            part = _dot(a_s[:, k * deep:(k + 1) * deep], arrived(p + k))
            acc_s[...] = part if k == 0 else acc_s[...] + part
            issue(i, p + k + SLOTS, low + k + SLOTS, high + k + SLOTS)
        return acc_s[...].astype(BF16)

    def project_kv(i):
        at = pl.ds(pl.multiple_of(i * R, R), R)
        t = project(i, jnp.int32(0), 0, 1)
        for j in range(kv):
            k_s[j, at, :] = turned(t[:, j * HEAD:(j + 1) * HEAD])
            v_s[j, :HEAD, at] = t[:, (kv + j) * HEAD:(kv + j + 1) * HEAD].T

    def project_q(i, start, first, count):
        def tile(m, _):
            t = project(i, start + m * steps, start, start + (count - 1) * steps + 1)
            for h in range(TO // HEAD):
                q_s[pl.ds(pl.multiple_of(((first + m) * (TO // HEAD) + h) * R, R), R), :] = turned(t[:, h * HEAD:(h + 1) * HEAD])
            return None

        lax.fori_loop(0, count, tile, None)

    e = HEAD**-0.5 * LOG2E
    pieces = [(j, at) for j in range(kv) for at in range(0, cols, STRIP)]

    def attention(i):
        top_s[...] = jnp.full(top_s.shape, NEG, F32)
        mix_s[...] = jnp.zeros(mix_s.shape, F32)

        def block(b, masked):
            here = pl.ds(pl.multiple_of(b * R, R), R)
            scores = [_dot(k_s[j, here, :], q_s[j * cols + at:j * cols + at + STRIP, :], 1, 1) for j, at in pieces]
            if masked:
                query = lax.rem(lax.broadcasted_iota(jnp.int32, (R, STRIP), 1), R)
                ok = query >= lax.broadcasted_iota(jnp.int32, (R, STRIP), 0)
            weights, keeps = [], []
            for (j, at), s in zip(pieces, scores):
                if masked:
                    s = jnp.where(ok, s, HIDDEN)
                old = top_s[j:j + 1, at:at + STRIP]
                top = jnp.maximum(old, s.max(axis=0, keepdims=True))
                top_s[j:j + 1, at:at + STRIP] = top
                weights.append(jnp.exp2((s - top) * e).astype(BF16))
                keeps.append(jnp.exp2((old - top) * e))
            for (j, at), p, keep in zip(pieces, weights, keeps):
                mix_s[j, :, at:at + STRIP] = mix_s[j, :, at:at + STRIP] * keep + _dot(v_s[j, :, here], p)

        lax.fori_loop(0, i, lambda b, _: block(b, False), None)
        block(i, True)
        slot = lax.rem(i, 3)
        for j in range(kv):
            share = 1 / mix_s[j, HEAD:HEAD + 1, :]
            for g in range(group):
                seen = mix_s[j, :HEAD, g * R:(g + 1) * R] * share[:, g * R:(g + 1) * R]
                seen_s[slot, :, (j * group + g) * HEAD:(j * group + g + 1) * HEAD] = seen.T.astype(BF16)

    def over_wo(i, first, start, before, body, after):
        j = i - first

        @pl.when(live(i, first))
        def _():
            before(j)

        def step(t, _):
            p = start + t

            @pl.when(live(i, first))
            def _():
                body(j, t, arrived(p))

            issue(i, p + SLOTS, start + SLOTS, start + tiles + SLOTS)
            return None

        lax.fori_loop(0, tiles, step, None)

        @pl.when(live(i, first))
        def _():
            after(j)

    def no_front(i, start, stop):
        @pl.when(i >= chunks)
        def _():
            for p in range(start + SLOTS, stop + SLOTS):
                issue(i, jnp.int32(p), p, p + 1)

    def nothing(j):
        pass

    def body_a(j, t, w):
        s, d, m = lax.rem(j, 2), lax.rem(t, 2), t // 2
        rs1s[s, d, m] = _dot(seen_s[lax.rem(j, 3)], w).astype(BF16)
        rs1(j, d, m).start()

    def half_done(j, t, adds):
        for d in range(2):
            @pl.when(t == (d + 1) * per - 1)
            def _():
                rs2(j, d, adds).start()

    def body_free(j, t, w):
        rs2s[lax.rem(j, 2), t // per, jnp.where(t < per, per, 0) + lax.rem(t, per)] = _dot(seen_s[lax.rem(j, 3)], w).astype(BF16)
        half_done(j, t, 0)

    def before_b(j):
        for d in range(2):
            for m in range(per):
                rs1(j, d, m).wait_recv()

    def body_b(j, t, w):
        d, m = t // per, lax.rem(t, per)
        rs2s[lax.rem(j, 2), d, t] = (_dot(seen_s[lax.rem(j, 3)], w) + rs1r[lax.rem(j, 4), d, m].astype(F32)).astype(BF16)
        half_done(j, t, 1)

    def before_c(j):
        residual(j).wait()
        for d in range(2):
            for adds in range(2):
                rs2(j, d, adds).wait_recv()

    def body_c(j, t, w):
        s, r = lax.rem(j, 2), lax.rem(j, 4)
        at = pl.ds(pl.multiple_of(t * TO, TO), TO)
        total = _dot(seen_s[lax.rem(j, 3)], w) + rs2r[r, 0, t].astype(F32) + rs2r[r, 1, t].astype(F32)
        yq[s, :, at] = (xres[:, at].astype(F32) + total).astype(BF16)

    def after_c(j):
        for d in range(2):
            ag1(j, d).start()
        own(j).start()

    def iteration(i, _):
        def when(first, do):
            @pl.when(live(i, first))
            def _():
                do(i - first)

        def a_sent(j):
            for d in range(2):
                for m in range(per):
                    rs1(j, d, m).wait_send()
                rs2(j, d, 0).wait_send()

        def b_sent(j):
            for d in range(2):
                rs2(j, d, 1).wait_send()

        def ag1_sent(j):
            for d in range(2):
                ag1(j, d).wait_send()
            own(j).wait()

        def forward(j):
            for d in range(2):
                ag1(j, d).wait_recv()
                ag2(j, d).start()

        def end(j):
            for d in range(2):
                ag2(j, d).wait()

        when(2, lambda j: residual(j).start())

        def front(j):
            table(j)
            norm(j)
            project_kv(j)
            project_q(j, at_q, 0, early)

        def rest(j):
            project_q(j, at_rest, early, columns_q - early)
            attention(j)

        when(0, front)
        no_front(i, 0, at_b)
        when(3, b_sent)
        over_wo(i, 1, at_b, before_b, body_b, nothing)
        when(2, a_sent)
        when(0, rest)
        no_front(i, at_rest, at_a)
        over_wo(i, 0, at_a, nothing, body_a, nothing)
        over_wo(i, 0, at_free, nothing, body_free, nothing)
        when(4, ag1_sent)
        over_wo(i, 2, at_c, before_c, body_c, after_c)
        when(3, forward)
        when(4, end)
        return None

    lax.fori_loop(0, chunks + 4, iteration, None)


def solution(mesh):
    n = mesh.shape["tp"]

    def step(x, gain, wq, wk, wv, wo):
        rows, width = x.shape
        half = HEAD // 2
        freq = THETA ** (-(np.arange(HEAD) % half) / half)
        kv, heads = wk.shape[1] // HEAD, wq.shape[1] // HEAD
        cols = heads // kv * R
        tiles = width // n // TO
        hbm, vmem = pl.BlockSpec(memory_space=pl.ANY), pl.BlockSpec(memory_space=pltpu.VMEM)
        dma = pltpu.SemaphoreType.DMA
        return pl.pallas_call(
            functools.partial(_kernel, n),
            out_shape=jax.ShapeDtypeStruct(x.shape, BF16),
            in_specs=[hbm, vmem, hbm, hbm, hbm, hbm, vmem],
            out_specs=hbm,
            scratch_shapes=[
                pltpu.VMEM((R, HEAD), F32),
                pltpu.VMEM((R, HEAD), F32),
                pltpu.VMEM((1, width), F32),
                pltpu.VMEM((SLOTS, wo.shape[0], TO), BF16),
                pltpu.VMEM((R, TO), F32),
                pltpu.VMEM((R, width), BF16),
                pltpu.VMEM((R, width // n), BF16),
                pltpu.VMEM((R, width), BF16),
                pltpu.VMEM((heads * R, HEAD), BF16),
                pltpu.VMEM((kv, rows, HEAD), BF16),
                pltpu.VMEM((kv, HEAD + ONES, rows), BF16),
                pltpu.VMEM((kv, cols), F32),
                pltpu.VMEM((kv, HEAD + ONES, cols), F32),
                pltpu.VMEM((3, R, heads * HEAD), BF16),
                pltpu.VMEM((2, 2, tiles // 2, R, TO), BF16),
                pltpu.VMEM((4, 2, tiles // 2, R, TO), BF16),
                pltpu.VMEM((2, 2, tiles, R, TO), BF16),
                pltpu.VMEM((4, 2, tiles, R, TO), BF16),
                pltpu.VMEM((2, R, width // n), BF16),
                dma((SLOTS,)), dma, dma, dma((2,)),
                dma((2, 2, tiles // 2)), dma((4, 2, tiles // 2)), dma((2, 2, 2)), dma((4, 2, 2)), dma((2, 2)), dma((4, 2)), dma((2, 2)), dma((4, 2)),
            ],
            compiler_params=pltpu.CompilerParams(collective_id=0, has_side_effects=True, vmem_limit_bytes=VMEM),
        )(x, gain.reshape(-1, 128), wq, wk, wv, wo, jnp.asarray(freq, F32)[None])

    tokens, columns = P("dp", None), P(None, "tp")
    return jax.shard_map(
        step,
        mesh=mesh,
        in_specs=(tokens, P(None), columns, columns, columns, P("tp", None)),
        out_specs=tokens,
        check_vma=False,
    )
```

```python
import functools

import jax
import jax.numpy as jnp
import numpy as np
from jax import lax
from jax.experimental import pallas as pl
from jax.experimental.pallas import tpu as pltpu
from jax.sharding import PartitionSpec as P

HEAD = 128
THETA = 10000
NEG = -1e30
HIDDEN = 2 * NEG
LOG2E = 1.4426950408889634
VMEM = 67043328
R = 256
TO = 512
SLOTS = 6
STRIP = 512
ONES = 16
F32, BF16 = jnp.float32, jnp.bfloat16


def _dot(a, b, ca=1, cb=0):
    return lax.dot_general(a, b, (((ca,), (cb,)), ((), ())), preferred_element_type=F32)


def _kernel(n, x, gain, wq, wk, wv, wo, freq, y,
            cos, sin, gain_s, wbuf, acc_s, xin, xres, a_s, q_s, k_s, v_s, top_s, mix_s, seen_s, rs1s, rs1r, rs2s, rs2r, yq,
            w_sem, x_sem, xres_sem, own_sem, rs1_ss, rs1_rs, rs2_ss, rs2_rs, ag1_ss, ag1_rs, ag2_ss, ag2_rs):
    rows, width = x.shape
    chunks = rows // R
    quarter = width // n
    half = quarter // 2
    tiles = quarter // TO
    per = tiles // 2
    deep = wo.shape[0]
    steps = width // deep
    kv = k_s.shape[0]
    group = q_s.shape[0] // (kv * R)
    cols = group * R
    me = lax.axis_index("tp")
    right, left, far = lax.rem(me + 1, n), lax.rem(me + n - 1, n), lax.rem(me + 2, n)
    to = (right, left)

    barrier = pltpu.get_barrier_semaphore()
    for neighbour in to:
        pl.semaphore_signal(barrier, inc=1, device_id={"tp": neighbour}, device_id_type=pl.DeviceIdType.MESH)

    def remote(src, dst, send, recv, d):
        return pltpu.make_async_remote_copy(src_ref=src, dst_ref=dst, send_sem=send, recv_sem=recv, device_id={"tp": jnp.where(d == 0, right, left)},
                                            device_id_type=pl.DeviceIdType.MESH)

    def place(j, column, size):
        return y.at[pl.ds(pl.multiple_of(j * R, R), R), pl.ds(pl.multiple_of(column, TO), size)]

    def rs1(j, d, m):
        s, r = lax.rem(j, 2), lax.rem(j, 4)
        return remote(rs1s.at[s, d, m], rs1r.at[r, d, m], rs1_ss.at[s, d, m], rs1_rs.at[r, d, m], d)

    def rs2(j, d, adds):
        s, r = lax.rem(j, 2), lax.rem(j, 4)
        at = pl.ds((d if adds else 1 - d) * per, per)
        return remote(rs2s.at[s, d, at], rs2r.at[r, d, at], rs2_ss.at[s, d, adds], rs2_rs.at[r, d, adds], d)

    def ag1(j, d):
        s, r = lax.rem(j, 2), lax.rem(j, 4)
        return remote(yq.at[s], place(j, me * quarter, quarter), ag1_ss.at[s, d], ag1_rs.at[r, d], d)

    def ag2(j, d):
        s, r = lax.rem(j, 2), lax.rem(j, 4)
        here = place(j, (left, right)[d] * quarter + d * half, half)
        return remote(here, here, ag2_ss.at[s, d], ag2_rs.at[r, d], d)

    def own(j):
        s = lax.rem(j, 2)
        return pltpu.make_async_copy(yq.at[s], place(j, me * quarter, quarter), own_sem.at[s])

    parts = x_sem.shape[0]
    some_rows = R // parts

    def chunk_of_x(j, n):
        at = pl.ds(n * some_rows, some_rows)
        return pltpu.make_async_copy(x.at[pl.ds(pl.multiple_of(j * R + n * some_rows, some_rows), some_rows), :], xin.at[at, :], x_sem.at[n])

    def residual(j):
        at = pl.ds(pl.multiple_of(j * R, R), R), pl.ds(pl.multiple_of(me * quarter, TO), quarter)
        return pltpu.make_async_copy(x.at[at], xres, xres_sem)

    columns_q = wq.shape[1] // TO
    early = columns_q // 2
    at_q = steps
    at_b = at_q + steps * early
    at_rest = at_b + tiles
    at_a = at_rest + steps * (columns_q - early)
    at_free = at_a + tiles
    at_c = at_free + tiles
    every = at_c + tiles

    def column_a(t):
        return far * quarter + (lax.rem(t, 2) * per + t // 2) * TO

    def column_free(t):
        return jnp.where(t < per, right, left) * quarter + (jnp.where(t < per, per, 0) + lax.rem(t, per)) * TO

    def column_b(t):
        return jnp.where(t < per, right, left) * quarter + t * TO

    def column_c(t):
        return me * quarter + t * TO

    def fetch(ref, row, column, dst, slot):
        pltpu.make_async_copy(ref.at[pl.ds(pl.multiple_of(row, 16), deep), pl.ds(pl.multiple_of(column, 128), dst.shape[1])], dst,
                              w_sem.at[slot]).start()

    def fetch_kv(t, slot):
        fetch(wk, t * deep, 0, wbuf.at[slot, :, :TO // 2], slot)
        fetch(wv, t * deep, 0, wbuf.at[slot, :, TO // 2:], slot)

    def fetch_q(first):
        return lambda t, slot: fetch(wq, lax.rem(t, steps) * deep, (first + t // steps) * TO, wbuf.at[slot], slot)

    def fetch_o(column):
        return lambda t, slot: fetch(wo, 0, column(t), wbuf.at[slot], slot)

    def live(i, first):
        return (i >= first) & (i < chunks + first)

    order = [(0, at_q, 0, fetch_kv), (at_q, at_b, 0, fetch_q(0)), (at_b, at_rest, 1, fetch_o(column_b)),
             (at_rest, at_a, 0, fetch_q(early)), (at_a, at_free, 0, fetch_o(column_a)), (at_free, at_c, 0, fetch_o(column_free)),
             (at_c, every, 2, fetch_o(column_c))]

    def issue(i, p, low, high):
        for later in range(2):
            for start, stop, first, do in order:
                start, stop = start + later * every, stop + later * every
                if start < high and stop > low:
                    @pl.when((p >= start) & (p < stop) & live(i + later, first))
                    def _():
                        do(p - start, lax.rem(p, SLOTS))

    def arrived(p):
        slot = lax.rem(p, SLOTS)
        pltpu.make_async_copy(wo.at[:, :TO], wbuf.at[slot], w_sem.at[slot]).wait()
        return wbuf[slot]

    for n in range(parts):
        chunk_of_x(0, n).start()
    for p in range(SLOTS):
        issue(jnp.int32(0), jnp.int32(p), p, p + 1)
    v_s[:, HEAD:, :] = jnp.ones((kv, ONES, rows), BF16)
    wide = gain[...].astype(F32)
    for c in range(width // 128):
        gain_s[:, c * 128:(c + 1) * 128] = wide[c:c + 1, :]
    pl.semaphore_wait(barrier, 2)

    def norm(i):
        part = 512

        def some(r, _):
            at = pl.ds(pl.multiple_of(r * 16, 16), 16)
            total = jnp.zeros((16, part), F32)
            for c in range(0, width, part):
                v = xin[at, c:c + part].astype(F32)
                total += v * v
            scale = lax.rsqrt(total.sum(axis=1, keepdims=True) * (1 / width) + 1e-6)
            for c in range(0, width, part):
                a_s[at, c:c + part] = (xin[at, c:c + part].astype(F32) * scale * gain_s[:, c:c + part]).astype(BF16)
            return None

        for n in range(parts):
            chunk_of_x(i, n).wait()
            lax.fori_loop(n * some_rows // 16, (n + 1) * some_rows // 16, some, None)

        @pl.when(i + 1 < chunks)
        def _():
            for n in range(parts):
                chunk_of_x(i + 1, n).start()

    def table(i):
        angle = (i * R + lax.broadcasted_iota(jnp.int32, (R, HEAD), 0)).astype(F32) * freq[...]
        low = lax.broadcasted_iota(jnp.int32, (R, HEAD), 1) < HEAD // 2
        sine = jnp.sin(angle)
        cos[...] = jnp.cos(angle)
        sin[...] = jnp.where(low, -sine, sine)

    def turned(t):
        t = t.astype(F32)
        return (t * cos[...] + pltpu.roll(t, HEAD // 2, 1) * sin[...]).astype(BF16)

    def project(i, p, low, high):
        for k in range(steps):
            part = _dot(a_s[:, k * deep:(k + 1) * deep], arrived(p + k))
            acc_s[...] = part if k == 0 else acc_s[...] + part
            issue(i, p + k + SLOTS, low + k + SLOTS, high + k + SLOTS)
        return acc_s[...].astype(BF16)

    def project_kv(i):
        at = pl.ds(pl.multiple_of(i * R, R), R)
        t = project(i, jnp.int32(0), 0, 1)
        for j in range(kv):
            k_s[j, at, :] = turned(t[:, j * HEAD:(j + 1) * HEAD])
            v_s[j, :HEAD, at] = t[:, (kv + j) * HEAD:(kv + j + 1) * HEAD].T

    def project_q(i, start, first, count):
        def tile(m, _):
            t = project(i, start + m * steps, start, start + (count - 1) * steps + 1)
            for h in range(TO // HEAD):
                q_s[pl.ds(pl.multiple_of(((first + m) * (TO // HEAD) + h) * R, R), R), :] = turned(t[:, h * HEAD:(h + 1) * HEAD])
            return None

        lax.fori_loop(0, count, tile, None)

    e = HEAD**-0.5 * LOG2E
    pieces = [(j, at) for j in range(kv) for at in range(0, cols, STRIP)]

    def attention(i):
        top_s[...] = jnp.full(top_s.shape, NEG, F32)
        mix_s[...] = jnp.zeros(mix_s.shape, F32)

        def block(b, masked):
            here = pl.ds(pl.multiple_of(b * R, R), R)
            scores = [_dot(k_s[j, here, :], q_s[j * cols + at:j * cols + at + STRIP, :], 1, 1) for j, at in pieces]
            if masked:
                query = lax.rem(lax.broadcasted_iota(jnp.int32, (R, STRIP), 1), R)
                ok = query >= lax.broadcasted_iota(jnp.int32, (R, STRIP), 0)
            weights, keeps = [], []
            for (j, at), s in zip(pieces, scores):
                if masked:
                    s = jnp.where(ok, s, HIDDEN)
                old = top_s[j:j + 1, at:at + STRIP]
                top = jnp.maximum(old, s.max(axis=0, keepdims=True))
                top_s[j:j + 1, at:at + STRIP] = top
                weights.append(jnp.exp2((s - top) * e).astype(BF16))
                keeps.append(jnp.exp2((old - top) * e))
            for (j, at), p, keep in zip(pieces, weights, keeps):
                mix_s[j, :, at:at + STRIP] = mix_s[j, :, at:at + STRIP] * keep + _dot(v_s[j, :, here], p)

        lax.fori_loop(0, i, lambda b, _: block(b, False), None)
        block(i, True)
        slot = lax.rem(i, 3)
        for j in range(kv):
            share = 1 / mix_s[j, HEAD:HEAD + 1, :]
            for g in range(group):
                seen = mix_s[j, :HEAD, g * R:(g + 1) * R] * share[:, g * R:(g + 1) * R]
                seen_s[slot, :, (j * group + g) * HEAD:(j * group + g + 1) * HEAD] = seen.T.astype(BF16)

    def over_wo(i, first, start, before, body, after):
        j = i - first

        @pl.when(live(i, first))
        def _():
            before(j)

        def step(t, _):
            p = start + t

            @pl.when(live(i, first))
            def _():
                body(j, t, arrived(p))

            issue(i, p + SLOTS, start + SLOTS, start + tiles + SLOTS)
            return None

        lax.fori_loop(0, tiles, step, None)

        @pl.when(live(i, first))
        def _():
            after(j)

    def no_front(i, start, stop):
        @pl.when(i >= chunks)
        def _():
            for p in range(start + SLOTS, stop + SLOTS):
                issue(i, jnp.int32(p), p, p + 1)

    def nothing(j):
        pass

    def body_a(j, t, w):
        s, d, m = lax.rem(j, 2), lax.rem(t, 2), t // 2
        rs1s[s, d, m] = _dot(seen_s[lax.rem(j, 3)], w).astype(BF16)
        rs1(j, d, m).start()

    def half_done(j, t, adds):
        for d in range(2):
            @pl.when(t == (d + 1) * per - 1)
            def _():
                rs2(j, d, adds).start()

    def body_free(j, t, w):
        rs2s[lax.rem(j, 2), t // per, jnp.where(t < per, per, 0) + lax.rem(t, per)] = _dot(seen_s[lax.rem(j, 3)], w).astype(BF16)
        half_done(j, t, 0)

    def before_b(j):
        for d in range(2):
            for m in range(per):
                rs1(j, d, m).wait_recv()

    def body_b(j, t, w):
        d, m = t // per, lax.rem(t, per)
        rs2s[lax.rem(j, 2), d, t] = (_dot(seen_s[lax.rem(j, 3)], w) + rs1r[lax.rem(j, 4), d, m].astype(F32)).astype(BF16)
        half_done(j, t, 1)

    def before_c(j):
        residual(j).wait()
        for d in range(2):
            for adds in range(2):
                rs2(j, d, adds).wait_recv()

    def body_c(j, t, w):
        s, r = lax.rem(j, 2), lax.rem(j, 4)
        at = pl.ds(pl.multiple_of(t * TO, TO), TO)
        total = _dot(seen_s[lax.rem(j, 3)], w) + rs2r[r, 0, t].astype(F32) + rs2r[r, 1, t].astype(F32)
        yq[s, :, at] = (xres[:, at].astype(F32) + total).astype(BF16)

    def after_c(j):
        for d in range(2):
            ag1(j, d).start()
        own(j).start()

    def iteration(i, _):
        def when(first, do):
            @pl.when(live(i, first))
            def _():
                do(i - first)

        def a_sent(j):
            for d in range(2):
                for m in range(per):
                    rs1(j, d, m).wait_send()
                rs2(j, d, 0).wait_send()

        def b_sent(j):
            for d in range(2):
                rs2(j, d, 1).wait_send()

        def ag1_sent(j):
            for d in range(2):
                ag1(j, d).wait_send()
            own(j).wait()

        def forward(j):
            for d in range(2):
                ag1(j, d).wait_recv()
                ag2(j, d).start()

        def end(j):
            for d in range(2):
                ag2(j, d).wait()

        when(2, lambda j: residual(j).start())

        def front(j):
            table(j)
            norm(j)
            project_kv(j)
            project_q(j, at_q, 0, early)

        def rest(j):
            project_q(j, at_rest, early, columns_q - early)
            attention(j)

        when(0, front)
        no_front(i, 0, at_b)
        when(3, b_sent)
        over_wo(i, 1, at_b, before_b, body_b, nothing)
        when(2, a_sent)
        when(0, rest)
        no_front(i, at_rest, at_a)
        over_wo(i, 0, at_a, nothing, body_a, nothing)
        over_wo(i, 0, at_free, nothing, body_free, nothing)
        when(4, ag1_sent)
        over_wo(i, 2, at_c, before_c, body_c, after_c)
        when(3, forward)
        when(4, end)
        return None

    lax.fori_loop(0, chunks + 4, iteration, None)


def solution(mesh):
    n = mesh.shape["tp"]

    def step(x, gain, wq, wk, wv, wo):
        rows, width = x.shape
        half = HEAD // 2
        freq = THETA ** (-(np.arange(HEAD) % half) / half)
        kv, heads = wk.shape[1] // HEAD, wq.shape[1] // HEAD
        cols = heads // kv * R
        tiles = width // n // TO
        hbm, vmem = pl.BlockSpec(memory_space=pl.ANY), pl.BlockSpec(memory_space=pltpu.VMEM)
        dma = pltpu.SemaphoreType.DMA
        return pl.pallas_call(
            functools.partial(_kernel, n),
            out_shape=jax.ShapeDtypeStruct(x.shape, BF16),
            in_specs=[hbm, vmem, hbm, hbm, hbm, hbm, vmem],
            out_specs=hbm,
            scratch_shapes=[
                pltpu.VMEM((R, HEAD), F32),
                pltpu.VMEM((R, HEAD), F32),
                pltpu.VMEM((1, width), F32),
                pltpu.VMEM((SLOTS, wo.shape[0], TO), BF16),
                pltpu.VMEM((R, TO), F32),
                pltpu.VMEM((R, width), BF16),
                pltpu.VMEM((R, width // n), BF16),
                pltpu.VMEM((R, width), BF16),
                pltpu.VMEM((heads * R, HEAD), BF16),
                pltpu.VMEM((kv, rows, HEAD), BF16),
                pltpu.VMEM((kv, HEAD + ONES, rows), BF16),
                pltpu.VMEM((kv, cols), F32),
                pltpu.VMEM((kv, HEAD + ONES, cols), F32),
                pltpu.VMEM((3, R, heads * HEAD), BF16),
                pltpu.VMEM((2, 2, tiles // 2, R, TO), BF16),
                pltpu.VMEM((4, 2, tiles // 2, R, TO), BF16),
                pltpu.VMEM((2, 2, tiles, R, TO), BF16),
                pltpu.VMEM((4, 2, tiles, R, TO), BF16),
                pltpu.VMEM((2, R, width // n), BF16),
                dma((SLOTS,)), dma((4,)), dma, dma((2,)),
                dma((2, 2, tiles // 2)), dma((4, 2, tiles // 2)), dma((2, 2, 2)), dma((4, 2, 2)), dma((2, 2)), dma((4, 2)), dma((2, 2)), dma((4, 2)),
            ],
            compiler_params=pltpu.CompilerParams(collective_id=0, has_side_effects=True, vmem_limit_bytes=VMEM),
        )(x, gain.reshape(-1, 128), wq, wk, wv, wo, jnp.asarray(freq, F32)[None])

    tokens, columns = P("dp", None), P(None, "tp")
    return jax.shard_map(
        step,
        mesh=mesh,
        in_specs=(tokens, P(None), columns, columns, columns, P("tp", None)),
        out_specs=tokens,
        check_vma=False,
    )
```
